128 devices in a mesh: row: 16 (over z, x), col: 8 (over y, core).
Axes of the slice: x: 4, y: 4, z: 4, core: 2. Of those that a mesh axis runs over, the one named last changes fastest.
Arguments:
- tokens: bfloat16 [1024, 12288], P('col', 'row'), may hold values from -16 to 16
- norm_gain: float32 [12288], P('row'), may hold values from 0.25 to 1.75
- weight_in: bfloat16 [12288, 49152], P('row', 'col'), may hold values from -0.0546875 to 0.0546875
- weight_out: bfloat16 [49152, 12288], P('col', 'row'), may hold values from -0.02734375 to 0.02734375
Outputs:
- mixed: bfloat16 [1024, 12288], P('col', 'row')
The draws below stay inside these ranges and needn't reach their ends.
All inputs are finite; a program needn't handle non-finite values.
Results may differ from the reference program's by a relative error of at most 0.0051.
Values may be sent and summed in bfloat16 or wider, within the bound.
No kernel may reach another device: no remote copies, remote signals or barrier semaphores. Data moves between devices by JAX's collectives and lax.ppermute only.
A program may use at most 128 MiB of HBM per device.

```python
import math
import jax
import jax.numpy as jnp
from jax import lax

D = 12288
FF = 49152
TOKENS = 1024


def draw_tokens(key, part):
    base_key = jax.random.fold_in(key, 17)
    noise_key, col_key, row_key = jax.random.split(base_key, 3)
    position = jnp.arange(D, dtype=jnp.float32) / D
    col_scale = jnp.exp(math.log(3.0) * position + jax.random.uniform(col_key, (D,), jnp.float32, 0.0, math.log(3.0))) / 3.0
    row_scale = jnp.exp(jax.random.uniform(row_key, (TOKENS, 1), jnp.float32, math.log(0.1), 0.0))
    values = jax.random.normal(noise_key, (TOKENS, D), jnp.float32)
    return jnp.clip(values * row_scale * col_scale[None, :], -16.0, 16.0).astype(jnp.bfloat16)


def block_levels(rng, dims, pieces, smallest, largest):
    factor_of, own = 1.0, jax.random.fold_in(rng, 6)
    for dim, blocks in pieces:
        heights = jnp.exp(jax.random.uniform(jax.random.fold_in(own, dim), (blocks,), jnp.float32, smallest / len(pieces), largest / len(pieces)))
        factor_of = factor_of * jnp.repeat(heights, dims[dim] // blocks).reshape([-1 if axis == dim else 1 for axis in range(len(dims))])
    return factor_of


def centred(rng, dims, deviation, limit, cuts=(), held_as=jnp.bfloat16):
    factor_of = block_levels(rng, dims, cuts, -0.22, 0.18) if cuts else 1.0
    result = jax.random.normal(rng, dims, jnp.float32) * deviation * factor_of
    return jnp.minimum(jnp.maximum(result, -limit), limit).astype(held_as)


def setup_inputs(seed: int = 0) -> dict:
    key_of = jax.random.split(jax.random.key(seed), 5)
    tokens = draw_tokens(jax.random.fold_in(key_of[4], 71), 0)
    norm_gain = jnp.clip(1.0 + 0.15 * jax.random.normal(key_of[1], (D,), jnp.float32), 0.25, 1.75)
    weight_in = centred(key_of[2], (D, FF), D ** -0.5, 0.0546875, ((0, 16), (1, 8)))
    weight_out = centred(key_of[3], (FF, D), FF ** -0.5, 0.02734375, ((0, 8), (1, 16)))
    return {"tokens": tokens, "norm_gain": norm_gain, "weight_in": weight_in, "weight_out": weight_out}


epsilon = 1e-05

def reference(tokens, norm_gain, weight_in, weight_out):
    wide_input = tokens.astype(jnp.float32)
    scaled = (wide_input * norm_gain.astype(jnp.float32)[None, :]).astype(jnp.bfloat16)
    squares = lax.optimization_barrier(jnp.sum(wide_input * wide_input, axis=1))
    inverse = lax.rsqrt(squares / D + epsilon)
    hidden = jnp.dot(scaled, weight_in, preferred_element_type=jnp.float32) * inverse[:, None]
    active = jax.nn.gelu(hidden, approximate=True).astype(jnp.bfloat16)
    branch = jnp.dot(active, weight_out, preferred_element_type=jnp.float32)
    return (wide_input + branch).astype(jnp.bfloat16)
```

```python
import jax
import jax.numpy as jnp
from jax import lax
from jax.sharding import PartitionSpec as P

D = 12288
epsilon = 1e-05
F32, BF16 = jnp.float32, jnp.bfloat16


def shift_x(v, s):
    return lax.ppermute(v, "row", [(z * 4 + x, z * 4 + (x + s) % 4) for z in range(4) for x in range(4)])


def shift_z(v, s):
    return lax.ppermute(v, "row", [(z * 4 + x, (z + s) % 4 * 4 + x) for z in range(4) for x in range(4)])


def shift_y(v, s):
    return lax.ppermute(v, "col", [(y * 2 + k, (y + s) % 4 * 2 + k) for y in range(4) for k in range(2)])


def swap_core(v):
    return lax.ppermute(v, "col", [(y * 2 + k, y * 2 + 1 - k) for y in range(4) for k in range(2)])


def dot(a, b):
    return jnp.dot(a, b, preferred_element_type=F32)


def rows(v, index, size):
    return lax.dynamic_slice_in_dim(v, index * size, size, 0)


def reduce_color(xa, xb, weight_in, base, width, shift1, i1, shift2, i2):
    def w(step):
        return lax.dynamic_slice_in_dim(weight_in, base + (i1 + step) % 4 * width, width, 1)

    w2, wp, wm, wo = w(2), w(1), w(3), w(0)
    r1 = shift1(dot(xa, w2).astype(BF16), 1)
    l1 = shift1(dot(xb, w2).astype(BF16), -1)
    r2 = shift1(dot(xb, wp).astype(BF16), 1)
    l2 = shift1(dot(xa, wm).astype(BF16), -1)
    r3 = shift1((dot(xa, wp) + r1.astype(F32)).astype(BF16), 1)
    l3 = shift1((dot(xb, wm) + l1.astype(F32)).astype(BF16), -1)
    sa = dot(xa, wo) + l2.astype(F32) + r3.astype(F32)
    sb = dot(xb, wo) + r2.astype(F32) + l3.astype(F32)
    total = jnp.concatenate([sa, sb], axis=0)
    quarter = total.shape[0] // 4
    half = quarter // 2
    far = rows(total, (i2 + 2) % 4, quarter).astype(BF16)
    p1 = shift2(far[:half], 1)
    m1 = shift2(far[half:], -1)
    up = rows(total, (i2 + 1) % 4, quarter)
    down = rows(total, (i2 + 3) % 4, quarter)
    up = jnp.concatenate([up[:half] + p1.astype(F32), up[half:]], axis=0).astype(BF16)
    down = jnp.concatenate([down[:half], down[half:] + m1.astype(F32)], axis=0).astype(BF16)
    p2 = shift2(up, 1)
    m2 = shift2(down, -1)
    return rows(total, i2, quarter) + p2.astype(F32) + m2.astype(F32)


def spread_color(active, weight_out, base, width, shift1, i1, shift2, i2):
    half = active.shape[0] // 2

    def w(step):
        return lax.dynamic_slice_in_dim(weight_out, base + (i1 + step) % 4 * width, width, 0)

    before = shift2(active, 1)
    after = shift2(active, -1)
    far_top = shift2(before[:half], 1)
    far_low = shift2(after[half:], -1)
    ha = jnp.concatenate([before, active], axis=0)
    xa = shift1(ha, 1)
    ya = shift1(ha, -1)
    hb = jnp.concatenate([after, far_top, far_low], axis=0)
    xb = shift1(hb, 1)
    yb = shift1(hb, -1)
    ua = shift1(xa, 1)
    ub = shift1(yb, -1)
    wo, wl, wr, wf = w(0), w(3), w(1), w(2)
    ra = dot(ha, wo) + dot(xa, wl) + dot(ya, wr) + dot(ua, wf)
    rb = dot(hb, wo) + dot(xb, wl) + dot(yb, wr) + dot(ub, wf)
    return jnp.concatenate([rb, ra], axis=0)


def per_device(tokens, norm_gain, weight_in, weight_out):
    r, c = lax.axis_index("row"), lax.axis_index("col")
    z, x = r // 4, r % 4
    n = tokens.shape[0]
    half = n // 2
    before = shift_y(tokens, 1)
    after = shift_y(tokens, -1)
    far_top = shift_y(before[:half], 1)
    far_low = shift_y(after[half:], -1)
    mine = jnp.concatenate([tokens, before, after, far_top, far_low], axis=0)
    other = swap_core(mine)

    def prepare(v):
        wide = v.astype(F32)
        return (wide * norm_gain[None, :]).astype(BF16), jnp.sum(wide * wide, axis=1)

    xa, qa = prepare(mine)
    xb, qb = prepare(other)
    square = jnp.concatenate([qa, qb]).reshape(8, n)
    square = square + shift_x(square, 1) + shift_x(square, -1) + shift_x(square, 2)
    square = square + shift_z(square, 1) + shift_z(square, -1) + shift_z(square, 2)
    inverse = lax.rsqrt(square / D + epsilon).reshape(8 * n)

    columns = weight_in.shape[1]
    width = columns // 8
    colors = ((0, shift_x, x, shift_z, z), (columns // 2, shift_z, z, shift_x, x))
    branch = 0.0
    for base, shift1, i1, shift2, i2 in colors:
        hidden = reduce_color(xa, xb, weight_in, base, width, shift1, i1, shift2, i2)
        hidden = hidden * rows(inverse, i2, 2 * n)[:, None]
        active = jax.nn.gelu(hidden, approximate=True).astype(BF16)
        part = spread_color(active, weight_out, base, width, shift1, i1, shift2, i2)
        quarters = [rows(part, (q - i2 - 1) % 4, 2 * n) for q in range(4)]
        branch = branch + jnp.concatenate(quarters, axis=0)
    total = branch[: 4 * n] + swap_core(branch[4 * n :].astype(BF16)).astype(F32)
    far = total[3 * n :].astype(BF16)
    p1 = shift_y(far[:half], 1)
    m1 = shift_y(far[half:], -1)
    down, up = total[n : 2 * n], total[2 * n : 3 * n]
    up = jnp.concatenate([up[:half] + p1.astype(F32), up[half:]], axis=0).astype(BF16)
    down = jnp.concatenate([down[:half], down[half:] + m1.astype(F32)], axis=0).astype(BF16)
    p2 = shift_y(up, 1)
    m2 = shift_y(down, -1)
    result = total[:n] + p2.astype(F32) + m2.astype(F32)
    return (tokens.astype(F32) + result).astype(BF16)


def solution(mesh):
    in_specs = (P("col", "row"), P("row"), P("row", "col"), P("col", "row"))
    return jax.shard_map(per_device, mesh=mesh, in_specs=in_specs, out_specs=P("col", "row"), check_vma=False)
```
